256 devices in a mesh: seq: 2 (over core), vocab: 128 (over y, z, x).
Axes of the slice: x: 4, y: 4, z: 8, core: 2. Of those that a mesh axis runs over, the one named last changes fastest.
Arguments:
- hidden: bfloat16 [1024, 8192], P('seq', 'vocab'), may hold values from -80 to 80
- weight: bfloat16 [8192, 65536], P('seq', 'vocab'), may hold values from -0.06629126 to 0.06629126, as said below
- tangent: bfloat16 [8192, 65536], P('seq', 'vocab'), may hold values from -0.0625 to 0.0625
- targets: int32 [1024], P('seq'), may hold values from 0 to 65535
Outputs:
- ggn: bfloat16 [8192, 65536], P('seq', 'vocab')
- token_loss: float32 [1024], P('seq')
The draws below stay inside these ranges and needn't reach their ends.
Inputs may be any that keep to these rules, and one draw needn't show every extreme that they name: `weight`: entries of standard deviation about 8192 ** -0.5.
All inputs are finite; a program needn't handle non-finite values.
Results may differ from the reference program's by a relative error of at most 0.0065.
Values may be sent and summed in bfloat16 or wider, within the bound.
A program may use at most 64 MiB of HBM per device.

```python
import math
import jax
import jax.numpy as jnp
from jax import lax

D = 8192
V_DEV = 512
VOCAB = 65536
TOKENS = 1024
N_VOCAB = 128


def joint_weight(key):
    limit = 6.0 / math.sqrt(D)
    raw = jax.random.normal(jax.random.fold_in(key, 101), (D, VOCAB), jnp.float32) / math.sqrt(D)
    return jnp.clip(raw, -limit, limit)


def draw_weight(key, part):
    return joint_weight(key).astype(jnp.bfloat16)


def draw_hidden(key, part):
    hidden_key = jax.random.fold_in(key, 202)
    normal_part = 3.0 * jax.random.normal(hidden_key, (TOKENS, D), jnp.float32)
    return normal_part.astype(jnp.bfloat16)


def set_ends(result, stream_key, low, top_value):
    longest = result.shape.index(max(result.shape))
    spots = []
    for shift in (0, 1):
        where = [jax.random.randint(jax.random.fold_in(stream_key, axis), (), 0, length) for axis, length in enumerate(result.shape)]
        where[longest] = (where[longest] + shift) % result.shape[longest]
        spots.append(tuple(where))
    return result.at[spots[0]].set(low).at[spots[1]].set(top_value)


def shard_levels(stream_key, dims, cuts, smallest, high):
    gain, own = 1.0, jax.random.fold_in(stream_key, 6)
    for axis_at, blocks in cuts:
        steps = jnp.exp(jax.random.uniform(jax.random.fold_in(own, axis_at), (blocks,), jnp.float32, smallest / len(cuts), high / len(cuts)))
        gain = gain * jnp.repeat(steps, dims[axis_at] // blocks).reshape([-1 if axis == axis_at else 1 for axis in range(len(dims))])
    return gain


def normal_values(stream_key, dims, deviation, most, split=(), held_as=jnp.bfloat16):
    values = jax.random.normal(stream_key, dims, jnp.float32) * deviation
    if len(split) > 0:
        values = shard_levels(stream_key, dims, split, -0.22, 0.18) * values
    return jnp.clip(values, min=-most, max=most).astype(held_as)


def setup_inputs(seed: int = 0) -> dict:
    splits = jax.random.split(jax.random.key(seed), 5)
    hidden = draw_hidden(jax.random.fold_in(splits[4], 71), 0)
    weight = draw_weight(jax.random.fold_in(splits[4], 71), 0)
    tangent = normal_values(splits[2], (D, VOCAB), D ** -0.5, 0.0625, ((0, 2), (1, 128)))
    targets = set_ends(jax.random.randint(splits[3], (TOKENS,), 0, VOCAB), jax.random.fold_in(splits[3], 1), 0, VOCAB - 1).astype(jnp.int32)
    return dict(hidden=hidden, weight=weight, tangent=tangent, targets=targets)


def reference(hidden, weight, tangent, targets):
    logits = jnp.dot(hidden, weight, preferred_element_type=jnp.float32)
    tangent_logits = jnp.dot(hidden, tangent, preferred_element_type=jnp.float32)
    row_top = jnp.max(logits, axis=1, keepdims=True)
    exp_logits = jnp.exp(logits - row_top)
    totals = jnp.sum(exp_logits, axis=1, keepdims=True)
    expect = jnp.sum(exp_logits * tangent_logits, axis=1, keepdims=True) / totals
    columns = jnp.arange(VOCAB, dtype=jnp.int32)
    picked = jnp.sum(jnp.where(columns[None, :] == targets[:, None], logits, jnp.float32(0.0)), axis=1)
    token_loss = row_top[:, 0] + jnp.log(totals[:, 0]) - picked
    weight_term = (exp_logits / totals * (tangent_logits - expect)).astype(jnp.bfloat16)
    blocked = weight_term.reshape(TOKENS, N_VOCAB, V_DEV).transpose(1, 0, 2)

    def one_block(term_block):
        return jnp.einsum("td,tv->dv", hidden.astype(jnp.float32), term_block.astype(jnp.float32)).astype(jnp.bfloat16)

    pieces = lax.map(one_block, blocked)
    ggn = pieces.transpose(1, 0, 2).reshape(D, VOCAB)
    return ggn, token_loss
```

```python
import functools

import jax
import jax.numpy as jnp
from jax import lax
from jax.experimental import pallas as pl
from jax.experimental.pallas import tpu as pltpu
from jax.sharding import Mesh
from jax.sharding import PartitionSpec as P

VOCAB = ("vocab_0", "vocab_1", "vocab_2")
MESH = pl.DeviceIdType.MESH
F32, BF16 = jnp.float32, jnp.bfloat16
GROUPS, LANES, ROWS, WIDTH, HALF = 4, 128, 64, 512, 4096
CUTS = ((16, 32), (16, 48), (16, 32), (32, 48))
PLANE, LINE_Z, RING_Z, FAR_Z, LINE_Y, RING_X, FAR_X, LINE_X, RING_Y, FAR_Y = range(10)
ORDER = (
    (0, 0), (1, 0), (0, 1), (0, 2), (1, 1), (0, 3), (5, 0, 0, -1), (2, 0, 1, -1), (5, 0, 0, 1), (8, 0, 0, -1), (8, 0,
    0, 1), (4, 0, 3), (7, 0, 3), (1, 2), (2, 1, 1, -1), (4, 0, 1), (8, 1, 0, -1), (4, 0, 2), (5, 1, 0, -1), (2, 2, 1,
    -1), (8, 1, 0, 1), (7, 0, 2), (4, 1, 3), (7, 1, 3), (2, 0, 1, 1), (1, 3), (7, 0, 1), (5, 0, 3, -1), (2, 1, 1, 1),
    (5, 2, 0, -1), (5, 1, 0, 1), (8, 0, 3, -1), (2, 3, 1, -1), (4, 1, 2), (6, 0, 0), (7, 2, 3), (2, 2, 1, 1), (9, 0,
    0), (4, 1, 1), (8, 2, 0, -1), (2, 0, 2, -1), (5, 0, 1, -1), (7, 1, 1), (4, 2, 3), (7, 1, 2), (2, 1, 2, -1), (8, 1,
    3, -1), (5, 0, 2, -1), (5, 0, 3, 1), (8, 0, 3, 1), (2, 3, 1, 1), (5, 2, 0, 1), (2, 2, 2, -1), (8, 0, 2, -1), (5,
    1, 3, -1), (9, 1, 0), (8, 3, 0, -1), (5, 3, 0, -1), (2, 0, 2, 1), (8, 2, 0, 1), (4, 3, 3), (7, 3, 3), (2, 1, 2,
    1), (4, 2, 1), (7, 2, 2), (8, 0, 1, -1), (4, 2, 2), (2, 3, 2, -1), (7, 2, 1), (5, 1, 2, -1), (2, 2, 2, 1), (8, 1,
    3, 1), (5, 0, 1, 1), (5, 2, 3, -1), (2, 0, 3, -1), (6, 1, 0), (5, 0, 2, 1), (8, 0, 2, 1), (2, 1, 3, -1), (8, 2, 3,
    -1), (5, 1, 1, -1), (8, 3, 0, 1), (8, 1, 1, -1), (2, 3, 2, 1), (5, 1, 3, 1), (2, 2, 3, -1), (8, 1, 2, -1), (5, 3,
    0, 1), (6, 2, 0), (4, 3, 1), (2, 0, 3, 1), (5, 3, 3, -1), (4, 3, 2), (5, 2, 1, -1), (6, 0, 3), (9, 0, 3), (7, 3,
    1), (2, 3, 3, -1), (9, 2, 0), (5, 2, 2, -1), (8, 3, 3, -1), (2, 1, 3, 1), (8, 0, 1, 1), (7, 3, 2), (2, 2, 3, 1),
    (8, 2, 3, 1), (6, 0, 2), (8, 2, 2, -1), (5, 1, 2, 1), (8, 1, 1, 1), (5, 2, 3, 1), (8, 1, 2, 1), (5, 3, 1, -1), (6,
    0, 1), (6, 1, 3), (8, 2, 1, -1), (9, 3, 0), (5, 3, 2, -1), (9, 1, 3), (6, 3, 0), (2, 3, 3, 1), (5, 1, 1, 1), (3,
    0), (3, 1), (9, 0, 2), (8, 3, 3, 1), (9, 0, 1), (5, 3, 3, 1), (8, 3, 1, -1), (6, 1, 2), (5, 2, 1, 1), (3, 2), (8,
    2, 2, 1), (6, 1, 1), (6, 2, 3), (8, 3, 2, -1), (5, 2, 2, 1), (9, 1, 1), (8, 2, 1, 1), (9, 2, 3), (9, 3, 3), (9, 1,
    2), (5, 3, 1, 1), (8, 3, 1, 1), (6, 3, 3), (5, 3, 2, 1), (6, 2, 1), (3, 3), (6, 2, 2), (8, 3, 2, 1), (9, 2, 2),
    (6, 3, 2), (9, 2, 1), (6, 3, 1), (9, 3, 2), (9, 3, 1),
)


class Gather:
    def __init__(self, block, held, lent, send_sems, recv_sems, far_sems):
        self.block, self.held, self.lent = block, held, lent
        self.send_sems, self.recv_sems, self.far_sems = send_sems, recv_sems, far_sems
        self.core, self.y, self.z, self.x = (lax.axis_index(a) for a in ("seq",) + VOCAB)
        self.names, self.far_names, self.sent, self.begun = {}, {}, 0, []
        self.left = {}
        for kind, group, *_ in ORDER:
            part = self.part(kind)
            self.left[group, part] = self.left.get((group, part), 0) + 1

    @staticmethod
    def part(kind):
        if kind in (PLANE, RING_Z, FAR_Z):
            return 0
        return 1 if kind in (LINE_Y, RING_X, FAR_X) else 2

    def rows(self, group, part):
        ends = (0, *CUTS[group], ROWS)
        return pl.ds(ends[part], ends[part + 1] - ends[part])

    def near(self, axis, step):
        at, count = {"y": (self.y, 4), "z": (self.z, 8), "x": (self.x, 4)}[axis]
        return lax.rem(at + step + count, count)

    def chip(self, **steps):
        return (self.core, *(self.near(a, steps.get(a, 0)) for a in "yzx"))

    def arrival(self, *name):
        if name not in self.names:
            self.names[name] = len(self.names)
        return self.recv_sems.at[self.names[name]]

    def departure(self):
        self.sent += 1
        return self.send_sems.at[self.sent - 1]

    def send(self, source, target, name, device, departure=None):
        copy = pltpu.make_async_remote_copy(
            src_ref=source,
            dst_ref=target,
            send_sem=self.departure() if departure is None else departure,
            recv_sem=self.arrival(*name),
            device_id=device,
            device_id_type=MESH,
        )
        copy.start()
        if departure is None:
            self.begun.append(copy)

    def take(self, ref, *name):
        pltpu.make_async_copy(ref, ref, self.arrival(*name)).wait()

    def ring(self, ref, axis, kind, group, piece, steps=(1, -1)):
        for step in steps:
            self.send(ref, ref, (kind, group, piece, step), self.chip(**{axis: step}))

    def start(self):
        self.lines = []
        for group in range(GROUPS):
            rest = pl.ds(CUTS[group][0], ROWS - CUTS[group][0])
            source = self.block.at[group, rest]
            target = self.held.at[group, self.y, self.z, self.x, rest]
            sem = self.departure()
            for step in (4, 3, 5, 2, 6, 1, 7):
                self.send(source, target, (LINE_Z, group), self.chip(z=step), sem)
            pltpu.make_async_copy(source, target, self.arrival(LINE_Z, group)).start()
            self.lines.append((self.held.at[group, 0, 0:7, 0, rest], sem))
            first = self.rows(group, 0)
            source = self.block.at[group, first]
            target = self.held.at[group, self.y, self.z, self.x, first]
            sem = self.departure()
            for dy in (2, 1, 3, 0):
                for dx in (2, 1, 3, 0):
                    if dy or dx:
                        self.send(source, target, (PLANE, group), self.chip(y=dy, x=dx), sem)
            pltpu.make_async_copy(source, target, self.arrival(PLANE, group)).start()
            self.lines.append((self.held.at[group, 0:3, 0:5, 0, first], sem))

    def event(self, kind, group, piece=0, step=0):
        held = self.held
        rows = self.rows(group, self.part(kind))
        if kind == PLANE:
            ref = held.at[group, :, self.z, :, rows]
            self.take(ref, PLANE, group)
            self.ring(ref, "z", RING_Z, group, 1)
        elif kind == LINE_Z:
            rest = pl.ds(CUTS[group][0], ROWS - CUTS[group][0])
            self.take(held.at[group, self.y, :, self.x, rest], LINE_Z, group)
            along_x = held.at[group, self.y, :, self.x, self.rows(group, 1)]
            along_y = held.at[group, self.y, :, self.x, self.rows(group, 2)]
            self.ring(along_y, "y", RING_Y, group, 0)
            self.ring(along_x, "x", RING_X, group, 0)
            for hop in (2, 1, 3):
                self.send(along_y, along_y, (LINE_X, group, hop), self.chip(x=hop))
                self.send(along_x, along_x, (LINE_Y, group, hop), self.chip(y=hop))
        elif kind == RING_Z:
            ref = held.at[group, :, self.near("z", -step * piece), :, rows]
            self.take(ref, RING_Z, group, piece, step)
            if piece < 3:
                self.ring(ref, "z", RING_Z, group, piece + 1, (step,))
            else:
                pl.when(lax.rem(self.core + group, 2) == (0 if step == 1 else 1))(
                    functools.partial(self.far, ref, "z", (FAR_Z, group), step)
                )
        elif kind == FAR_Z:
            self.take(held.at[group, :, self.near("z", 4), :, rows], FAR_Z, group)
        elif kind == LINE_Y:
            ref = held.at[group, self.near("y", -piece), :, self.x, rows]
            self.take(ref, LINE_Y, group, piece)
            self.ring(ref, "x", RING_X, group, piece)
        elif kind == LINE_X:
            ref = held.at[group, self.y, :, self.near("x", -piece), rows]
            self.take(ref, LINE_X, group, piece)
            self.ring(ref, "y", RING_Y, group, piece)
        elif kind == RING_X:
            ref = held.at[group, self.near("y", -piece), :, self.near("x", -step), rows]
            self.take(ref, RING_X, group, piece, step)
            pl.when(lax.rem(self.core + group + piece, 2) == (0 if step == 1 else 1))(
                functools.partial(self.far, ref, "x", (FAR_X, group, piece), step)
            )
        elif kind == RING_Y:
            ref = held.at[group, self.near("y", -step), :, self.near("x", -piece), rows]
            self.take(ref, RING_Y, group, piece, step)
            pl.when(lax.rem(self.core + group + piece, 2) == (0 if step == 1 else 1))(
                functools.partial(self.far, ref, "y", (FAR_Y, group, piece), step)
            )
        elif kind == FAR_X:
            self.take(held.at[group, self.near("y", -piece), :, self.near("x", 2), rows], FAR_X, group, piece)
        elif kind == FAR_Y:
            self.take(held.at[group, self.near("y", 2), :, self.near("x", -piece), rows], FAR_Y, group, piece)
        part = self.part(kind)
        self.left[group, part] -= 1
        if self.left[group, part] == 0:
            self.lend(group, part)

    def far(self, ref, axis, name, step):
        copy = pltpu.make_async_remote_copy(
            src_ref=ref,
            dst_ref=ref,
            send_sem=self.far_sem(name),
            recv_sem=self.arrival(*name),
            device_id=self.chip(**{axis: step}),
            device_id_type=MESH,
        )
        copy.start()

    def far_sem(self, name):
        self.far_names.setdefault(name, len(self.far_names))
        return self.far_sems.at[self.far_names[name]]

    def lend(self, group, part):
        rows = self.rows(group, part)
        source = self.held.at[group, pl.ds(2 - 2 * self.core, 2), :, :, rows]
        target = self.lent.at[group, :, :, :, rows]
        self.send(source, target, ("lend", group, part), (1 - self.core, self.y, self.z, self.x))

    def complete(self, group):
        for part in range(3):
            self.take(self.lent.at[group, :, :, :, self.rows(group, part)], "lend", group, part)

    def finish(self):
        for ref, sem in self.lines:
            pltpu.make_async_copy(ref, ref, sem).wait()
        for copy in self.begun:
            copy.wait_send()
        for (kind, group, *_), at in self.far_names.items():
            rows = self.rows(group, self.part(kind))
            ref = self.held.at[group, :, 0, :, rows] if kind == FAR_Z else self.held.at[group, 0, :, 0, rows]
            pltpu.make_async_copy(ref, ref, self.far_sems.at[at]).wait()


def greet():
    core, y, z, x = (lax.axis_index(a) for a in ("seq",) + VOCAB)
    sem = pltpu.get_barrier_semaphore()

    def plane(i, carry):
        to = (core, lax.rem(y + i // 4, 4), z, lax.rem(x + lax.rem(i, 4), 4))
        pl.semaphore_signal(sem, inc=1, device_id=to, device_id_type=MESH)
        return carry

    def line(i, carry):
        pl.semaphore_signal(sem, inc=1, device_id=(core, y, lax.rem(z + i, 8), x), device_id_type=MESH)
        return carry

    pl.semaphore_signal(sem, inc=1, device_id=(1 - core, y, z, x), device_id_type=MESH)
    lax.fori_loop(1, 8, line, 0)
    lax.fori_loop(1, 16, plane, 0)
    pl.semaphore_wait(sem, 1 + 7 + 15)


def kernel(
    block, targets, weight, tangent, ggn, loss,
    held, lent, staged, turned, near_part, far_part, got_part, plane, line, terms, total, leaving,
    send_sems, recv_sems, far_sems, load_sems, store_sems, part_sems, plane_sems, line_sems, term_sems,
):
    core, y, z, x = (lax.axis_index(a) for a in ("seq",) + VOCAB)
    loads = [
        pltpu.make_async_copy(source, staged.at[k], load_sems.at[k]) for k, source in enumerate((weight, tangent))
    ]
    for copy in loads:
        copy.start()
    greet()
    net = Gather(block, held, lent, send_sems, recv_sems, far_sems)
    net.start()
    partner = (1 - core, y, z, x)
    copies = []

    def turn(first, last):
        def chunk(i, carry):
            k, j = i // 4, lax.rem(i, 4)
            rows = pl.ds(pl.multiple_of(i * 256, 256), 256)
            lanes = pl.ds(pl.multiple_of(j * 256, 256), 256)
            turned[k, 0:WIDTH, lanes] = staged[0, rows, :].T
            turned[k, WIDTH : 2 * WIDTH, lanes] = staged[1, rows, :].T
            return carry

        lax.fori_loop(first, last, chunk, 0)

    def logits(g):
        net.complete(g)
        near_part[g] = jnp.zeros_like(near_part[g])
        far_part[g] = jnp.zeros_like(far_part[g])

        def deep(i, carry):
            half, zs = i // 2, pl.ds(4 * lax.rem(i, 2), 4)
            own = held[g, 2 * core + half, zs].reshape(1024, LANES)
            other = lent[g, half, zs].reshape(1024, LANES)
            product = jnp.dot(turned[i], jnp.concatenate([own, other], axis=1), preferred_element_type=F32)
            near_part[g] += product[:, :LANES]
            far_part[g] += product[:, LANES:]
            return carry

        lax.fori_loop(0, 4, deep, 0)
        copy = pltpu.make_async_remote_copy(
            src_ref=far_part.at[g], dst_ref=got_part.at[g], send_sem=part_sems.at[0, g], recv_sem=part_sems.at[1, g],
            device_id=partner, device_id_type=MESH,
        )
        copy.start()
        copies.append(copy)
        return copy

    def own_stats(g, copy):
        copy.wait_recv()
        values = near_part[g, 0:WIDTH] + got_part[g, 0:WIDTH]
        top = jnp.max(values, axis=0, keepdims=True)
        base = (y * 32 + z * 4 + x) * WIDTH
        ids = lax.broadcasted_iota(jnp.int32, (WIDTH, LANES), 0) + base
        picked = jnp.sum(jnp.where(ids == targets[g : g + 1, :], values, 0.0), axis=0, keepdims=True)
        exps = jnp.exp(values - top)
        near_part[g, 0:WIDTH] = exps
        tangents = near_part[g, WIDTH : 2 * WIDTH] + got_part[g, WIDTH : 2 * WIDTH]
        near_part[g, WIDTH : 2 * WIDTH] = tangents
        plane[g, 0, 0:1, :] = top
        plane[g, 0, 1:2, :] = jnp.sum(exps, axis=0, keepdims=True)
        plane[g, 0, 2:3, :] = jnp.sum(exps * tangents, axis=0, keepdims=True)
        plane[g, 0, 3:4, :] = picked
        plane[g, 0, 4:8, :] = jnp.zeros((4, LANES), F32)

        def give(i, carry):
            pltpu.make_async_remote_copy(
                src_ref=plane.at[g, 0], dst_ref=plane.at[g, i], send_sem=plane_sems.at[0, g],
                recv_sem=plane_sems.at[1, g],
                device_id=(core, lax.rem(y + i // 4, 4), z, lax.rem(x + lax.rem(i, 4), 4)), device_id_type=MESH,
            ).start()
            return carry

        lax.fori_loop(1, 16, give, 0)

    def joined(ref):
        tops = ref[:, 0:1, :]
        top = jnp.max(tops, axis=0)
        scale = jnp.exp(tops - top[None])
        sums = [jnp.sum(ref[:, k : k + 1, :] * scale, axis=0) for k in (1, 2)]
        return top, *sums, jnp.sum(ref[:, 3:4, :], axis=0)

    def plane_stats(g):
        every = plane.at[g, 1:16]
        pltpu.make_async_copy(every, every, plane_sems.at[1, g]).wait()
        for k, row in enumerate(joined(plane.at[g])):
            line[g, 0, k : k + 1, :] = row
        line[g, 0, 4:8, :] = jnp.zeros((4, LANES), F32)

        def give(i, carry):
            pltpu.make_async_remote_copy(
                src_ref=line.at[g, 0], dst_ref=line.at[g, i], send_sem=line_sems.at[0, g],
                recv_sem=line_sems.at[1, g], device_id=(core, y, lax.rem(z + i, 8), x), device_id_type=MESH,
            ).start()
            return carry

        lax.fori_loop(1, 8, give, 0)

    def term(g):
        every = line.at[g, 1:8]
        pltpu.make_async_copy(every, every, line_sems.at[1, g]).wait()
        top, totals, tangent_sum, picked = joined(line.at[g])
        loss[g : g + 1, :] = top + jnp.log(totals) - picked
        scale = jnp.exp(plane[g, 0, 0:1, :] - top) / totals
        expect = tangent_sum / totals
        value = near_part[g, 0:WIDTH] * scale * (near_part[g, WIDTH : 2 * WIDTH] - expect)
        terms[g, 0] = value.T.astype(BF16)
        copy = pltpu.make_async_remote_copy(
            src_ref=terms.at[g, 0], dst_ref=terms.at[g, 1], send_sem=term_sems.at[0, g], recv_sem=term_sems.at[1, g],
            device_id=partner, device_id_type=MESH,
        )
        copy.start()
        copies.append(copy)
        return copy

    def product(i, groups):
        half, zs = i // 4, pl.ds(2 * lax.rem(i, 4), 2)
        left, right = [], []
        for g in groups:
            left += [held[g, 2 * core + half, zs].reshape(512, LANES), lent[g, half, zs].reshape(512, LANES)]
            right += [terms[g, 0], terms[g, 1]]
        left, right = jnp.concatenate(left, axis=1), jnp.concatenate(right, axis=0)
        return jnp.dot(left, right, preferred_element_type=F32)

    def early(i, carry):
        total[pl.ds(pl.multiple_of(i * 512, 512), 512)] = product(i, (0, 1, 2))
        return carry

    def last(i, carry):
        rows = pl.ds(pl.multiple_of(i * 512, 512), 512)
        slot = lax.rem(i, 2)
        out = pltpu.make_async_copy(leaving.at[slot], ggn.at[rows], store_sems.at[slot])
        pl.when(i >= 2)(out.wait)
        leaving[slot] = (total[rows] + product(i, (3,))).astype(BF16)
        out.start()
        return carry

    for copy in loads:
        copy.wait()
    turns = {0: (0, 4), 1: (4, 8), 2: (8, 12), 6: (12, 16)}
    parts, sent = {}, {}
    ready = 0
    for at, event in enumerate(ORDER):
        if at in turns:
            turn(*turns[at])
        net.event(*event)
        while ready < GROUPS and not any(net.left[ready, p] for p in range(3)):
            g = ready
            parts[g] = logits(g)
            if g >= 1:
                own_stats(g - 1, parts[g - 1])
            if g >= 2:
                plane_stats(g - 2)
            if g >= 3:
                sent[g - 3] = term(g - 3)
            ready += 1
    own_stats(3, parts[3])
    plane_stats(2)
    sent[1] = term(1)
    plane_stats(3)
    sent[2] = term(2)
    for g in range(3):
        sent[g].wait_recv()
    lax.fori_loop(0, 8, early, 0)
    sent[3] = term(3)
    sent[3].wait_recv()
    lax.fori_loop(0, 8, last, 0)
    for slot in range(2):
        pltpu.make_async_copy(leaving.at[slot], ggn.at[0:512], store_sems.at[slot]).wait()
    net.finish()
    for copy in copies:
        copy.wait_send()
    for g in range(GROUPS):
        for sems, ref in ((plane_sems, plane.at[g, 1:16]), (line_sems, line.at[g, 1:8])):
            pltpu.make_async_copy(ref, ref, sems.at[0, g]).wait()


def on_device(hidden, weight, tangent, targets):
    block = hidden.reshape(GROUPS, LANES, ROWS).transpose(0, 2, 1)
    vmem, hbm = pl.BlockSpec(memory_space=pltpu.VMEM), pl.BlockSpec(memory_space=pl.ANY)
    dma = pltpu.SemaphoreType.DMA
    ggn, loss = pl.pallas_call(
        kernel,
        out_shape=(
            jax.ShapeDtypeStruct((HALF, WIDTH), BF16),
            jax.ShapeDtypeStruct((GROUPS, LANES), F32),
        ),
        in_specs=[vmem, vmem, hbm, hbm],
        out_specs=(hbm, vmem),
        scratch_shapes=[
            pltpu.VMEM((GROUPS, 4, 8, 4, ROWS, LANES), BF16),
            pltpu.VMEM((GROUPS, 2, 8, 4, ROWS, LANES), BF16),
            pltpu.VMEM((2, HALF, WIDTH), BF16),
            pltpu.VMEM((4, 2 * WIDTH, 1024), BF16),
            pltpu.VMEM((GROUPS, 2 * WIDTH, LANES), F32),
            pltpu.VMEM((GROUPS, 2 * WIDTH, LANES), F32),
            pltpu.VMEM((GROUPS, 2 * WIDTH, LANES), F32),
            pltpu.VMEM((GROUPS, 16, 8, LANES), F32),
            pltpu.VMEM((GROUPS, 8, 8, LANES), F32),
            pltpu.VMEM((GROUPS, 2, LANES, WIDTH), BF16),
            pltpu.VMEM((HALF, WIDTH), F32),
            pltpu.VMEM((2, 512, WIDTH), BF16),
            dma((SENDS,)),
            dma((ARRIVALS,)),
            dma((FARS,)),
            dma((2,)),
            dma((2,)),
            dma((2, GROUPS)),
            dma((2, GROUPS)),
            dma((2, GROUPS)),
            dma((2, GROUPS)),
        ],
        compiler_params=pltpu.CompilerParams(
            collective_id=0, has_side_effects=True, vmem_limit_bytes=60 * 2**20
        ),
        name="head_product",
    )(block, targets.reshape(GROUPS, LANES), weight, tangent)
    return ggn, loss.reshape(-1)


SENDS, ARRIVALS, FARS = 168, 172, 36


def solution(mesh):
    split = Mesh(
        mesh.devices.reshape(mesh.shape["seq"], 4, 8, 4), ("seq", "vocab_0", "vocab_1", "vocab_2")
    )
    placed = (P("seq", VOCAB), P("seq", VOCAB), P("seq", VOCAB), P("seq"))
    return jax.shard_map(
        on_device,
        mesh=split,
        in_specs=placed,
        out_specs=(P("seq", VOCAB), P("seq")),
        check_vma=False,
    )
```

```python
import functools
import math

import jax
import jax.numpy as jnp
from jax import lax
from jax.experimental import pallas as pl
from jax.experimental.pallas import tpu as pltpu
from jax.sharding import Mesh
from jax.sharding import PartitionSpec as P

VOCAB = ("vocab_0", "vocab_1", "vocab_2")
MESH = pl.DeviceIdType.MESH
F32, BF16 = jnp.float32, jnp.bfloat16
GROUPS, LANES, ROWS, WIDTH, HALF = 4, 128, 64, 512, 4096
CUTS = ((16, 32), (16, 48), (16, 32), (32, 48))
PLANE, LINE_Z, RING_Z, FAR_Z, LINE_Y, RING_X, FAR_X, LINE_X, RING_Y, FAR_Y, LOGITS = range(11)
ORDER = (
    (0, 0), (1, 0), (0, 1), (0, 2), (1, 1), (4, 0, 3), (7, 0, 3), (0, 3), (8, 0, 0, -1), (5, 0, 0, -1), (2, 0, 1, -1),
    (4, 0, 1), (4, 0, 2), (7, 1, 3), (1, 2), (4, 1, 3), (2, 1, 1, -1), (7, 0, 2), (8, 0, 0, 1), (8, 1, 0, -1), (5, 1,
    0, -1), (7, 0, 1), (2, 2, 1, -1), (5, 0, 3, -1), (1, 3), (8, 0, 3, -1), (5, 0, 0, 1), (2, 0, 1, 1), (5, 0, 1, -1),
    (5, 0, 2, -1), (8, 1, 3, -1), (4, 1, 2), (2, 1, 1, 1), (7, 1, 1), (7, 1, 2), (4, 2, 3), (2, 3, 1, -1), (4, 1, 1),
    (7, 2, 3), (8, 1, 0, 1), (2, 2, 1, 1), (5, 2, 0, -1), (8, 2, 0, -1), (5, 1, 0, 1), (2, 0, 2, -1), (5, 0, 3, 1),
    (8, 0, 3, 1), (5, 1, 3, -1), (8, 0, 2, -1), (5, 0, 1, 1), (2, 1, 2, -1), (8, 1, 3, 1), (5, 0, 2, 1), (2, 3, 1, 1),
    (2, 2, 2, -1), (7, 3, 3), (8, 0, 1, -1), (4, 2, 1), (5, 3, 0, -1), (4, 2, 2), (4, 3, 3), (2, 0, 2, 1), (8, 3, 0,
    -1), (8, 2, 0, 1), (7, 2, 2), (2, 1, 2, 1), (2, 3, 2, -1), (5, 1, 2, -1), (8, 1, 1, -1), (7, 2, 1), (5, 2, 3, -1),
    (8, 0, 2, 1), (2, 2, 2, 1), (8, 1, 2, -1), (5, 2, 0, 1), (2, 0, 3, -1), (5, 1, 1, -1), (8, 2, 3, -1), (5, 1, 3,
    1), (2, 1, 3, -1), (8, 0, 1, 1), (2, 3, 2, 1), (2, 2, 3, -1), (5, 2, 1, -1), (7, 3, 1), (7, 3, 2), (8, 3, 3, -1),
    (4, 3, 1), (5, 3, 3, -1), (4, 3, 2), (2, 0, 3, 1), (5, 3, 0, 1), (5, 2, 2, -1), (8, 3, 0, 1), (8, 1, 1, 1), (2, 1,
    3, 1), (2, 3, 3, -1), (8, 1, 2, 1), (8, 2, 2, -1), (5, 1, 2, 1), (2, 2, 3, 1), (5, 2, 3, 1), (8, 2, 3, 1), (5, 3,
    1, -1), (8, 2, 1, -1), (5, 1, 1, 1), (5, 3, 2, -1), (3, 0), (3, 1), (8, 3, 3, 1), (8, 3, 1, -1), (2, 3, 3, 1), (3,
    2), (6, 0), (8, 3, 2, -1), (5, 2, 1, 1), (10, 0, 0), (5, 3, 3, 1), (3, 3), (8, 2, 2, 1), (5, 2, 2, 1), (10, 1, 0),
    (10, 0, 1), (10, 2, 0), (8, 2, 1, 1), (9, 0), (5, 3, 1, 1), (5, 3, 2, 1), (8, 3, 1, 1), (10, 3, 0), (8, 3, 2, 1),
    (6, 1), (9, 1), (6, 2), (6, 3), (10, 0, 2), (9, 2), (9, 3), (10, 1, 2), (10, 2, 1), (10, 1, 1), (10, 3, 1), (10,
    2, 2), (10, 3, 2),
)


class Gather:
    def __init__(self, block, held, lent, send_sems, recv_sems):
        self.block, self.held, self.lent = block, held, lent
        self.send_sems, self.recv_sems = send_sems, recv_sems
        self.core, self.y, self.z, self.x = (lax.axis_index(a) for a in ("seq",) + VOCAB)
        self.names, self.sent = {}, [0] * GROUPS
        self.left = {}
        for kind, group, *_ in ORDER:
            if kind == LOGITS:
                continue
            part = self.part(kind)
            self.left[group, part] = self.left.get((group, part), 0) + 1

    @staticmethod
    def part(kind):
        if kind in (PLANE, RING_Z, FAR_Z):
            return 0
        return 1 if kind in (LINE_Y, RING_X, FAR_X) else 2

    def rows(self, group, part):
        ends = (0, *CUTS[group], ROWS)
        return pl.ds(ends[part], ends[part + 1] - ends[part])

    def near(self, axis, step):
        at, count = {"y": (self.y, 4), "z": (self.z, 8), "x": (self.x, 4)}[axis]
        return lax.rem(at + step + count, count)

    def chip(self, **steps):
        return (self.core, *(self.near(a, steps.get(a, 0)) for a in "yzx"))

    def arrival(self, *name):
        if name not in self.names:
            self.names[name] = len(self.names)
        return self.recv_sems.at[self.names[name]]

    def send(self, source, target, name, device, cond=None, counted=True):
        group = name[1]
        copy = pltpu.make_async_remote_copy(
            src_ref=source,
            dst_ref=target,
            send_sem=self.send_sems.at[group],
            recv_sem=self.arrival(*name),
            device_id=device,
            device_id_type=MESH,
        )
        if counted:
            self.sent[group] += math.prod(target.shape[:-1])
        if cond is None:
            copy.start()
        else:
            pl.when(cond)(copy.start)

    def take(self, ref, *name):
        pltpu.make_async_copy(ref, ref, self.arrival(*name)).wait()

    def ring(self, ref, axis, kind, group, piece, steps=(1, -1)):
        for step in steps:
            self.send(ref, ref, (kind, group, piece, step), self.chip(**{axis: step}))

    def start(self):
        for group in range(GROUPS):
            lanes = pl.ds(group * LANES, LANES)
            rest = pl.ds(CUTS[group][0], ROWS - CUTS[group][0])
            source = self.block.at[rest, lanes]
            target = self.held.at[group, self.y, self.z, self.x, rest]
            for step in (4, 3, 5, 2, 6, 1, 7):
                self.send(source, target, (LINE_Z, group), self.chip(z=step))
            pltpu.make_async_copy(source, target, self.arrival(LINE_Z, group)).start()
            first = self.rows(group, 0)
            source = self.block.at[first, lanes]
            target = self.held.at[group, self.y, self.z, self.x, first]
            for dy in (2, 1, 3, 0):
                for dx in (2, 1, 3, 0):
                    if dy or dx:
                        self.send(source, target, (PLANE, group), self.chip(y=dy, x=dx))
            pltpu.make_async_copy(source, target, self.arrival(PLANE, group)).start()

    def event(self, kind, group, piece=0, step=0):
        held = self.held
        rows = self.rows(group, self.part(kind))
        if kind == PLANE:
            ref = held.at[group, :, self.z, :, rows]
            self.take(ref, PLANE, group)
            self.ring(ref, "z", RING_Z, group, 1)
        elif kind == LINE_Z:
            rest = pl.ds(CUTS[group][0], ROWS - CUTS[group][0])
            self.take(held.at[group, self.y, :, self.x, rest], LINE_Z, group)
            along_x = held.at[group, self.y, :, self.x, self.rows(group, 1)]
            along_y = held.at[group, self.y, :, self.x, self.rows(group, 2)]
            for hop in (2, 1, 3):
                self.send(along_y, along_y, (LINE_X, group, hop), self.chip(x=hop))
                self.send(along_x, along_x, (LINE_Y, group, hop), self.chip(y=hop))
            self.ring(along_y, "y", RING_Y, group, 0)
            self.ring(along_x, "x", RING_X, group, 0)
        elif kind == RING_Z:
            ref = held.at[group, :, self.near("z", -step * piece), :, rows]
            self.take(ref, RING_Z, group, piece, step)
            if piece < 3:
                self.ring(ref, "z", RING_Z, group, piece + 1, (step,))
            else:
                self.far(ref, "z", FAR_Z, group, 0, step)
        elif kind == FAR_Z:
            self.take(held.at[group, :, self.near("z", 4), :, rows], FAR_Z, group)
        elif kind == LINE_Y:
            ref = held.at[group, self.near("y", -piece), :, self.x, rows]
            self.take(ref, LINE_Y, group, piece)
            self.ring(ref, "x", RING_X, group, piece)
        elif kind == LINE_X:
            ref = held.at[group, self.y, :, self.near("x", -piece), rows]
            self.take(ref, LINE_X, group, piece)
            self.ring(ref, "y", RING_Y, group, piece)
        elif kind == RING_X:
            ref = held.at[group, self.near("y", -piece), :, self.near("x", -step), rows]
            self.take(ref, RING_X, group, piece, step)
            self.far(ref, "x", FAR_X, group, piece, step)
        elif kind == RING_Y:
            ref = held.at[group, self.near("y", -step), :, self.near("x", -piece), rows]
            self.take(ref, RING_Y, group, piece, step)
            self.far(ref, "y", FAR_Y, group, piece, step)
        elif kind == FAR_X:
            self.take(held.at[group, :, :, self.near("x", 2), rows], FAR_X, group)
        elif kind == FAR_Y:
            self.take(held.at[group, self.near("y", 2), :, :, rows], FAR_Y, group)
        part = self.part(kind)
        self.left[group, part] -= 1
        if self.left[group, part] == 0:
            self.lend(group, part)

    def far(self, ref, axis, kind, group, piece, step):
        this_way = lax.rem(self.core + group + piece, 2) == (0 if step == 1 else 1)
        self.send(ref, ref, (kind, group), self.chip(**{axis: step}), this_way, step == 1)

    def lend(self, group, part):
        rows = self.rows(group, part)
        source = self.held.at[group, pl.ds(2 - 2 * self.core, 2), :, :, rows]
        target = self.lent.at[group, :, :, :, rows]
        self.send(source, target, ("lend", group, part), (1 - self.core, self.y, self.z, self.x))

    def finish(self, ref):
        for group, lines in enumerate(self.sent):
            every = ref.at[0 : lines * LANES * 2 // (WIDTH * 4)]
            pltpu.make_async_copy(every, every, self.send_sems.at[group]).wait()


def greet():
    core, y, z, x = (lax.axis_index(a) for a in ("seq",) + VOCAB)
    sem = pltpu.get_barrier_semaphore()

    def plane(i, carry):
        to = (core, lax.rem(y + i // 4, 4), z, lax.rem(x + lax.rem(i, 4), 4))
        pl.semaphore_signal(sem, inc=1, device_id=to, device_id_type=MESH)
        return carry

    def line(i, carry):
        pl.semaphore_signal(sem, inc=1, device_id=(core, y, lax.rem(z + i, 8), x), device_id_type=MESH)
        return carry

    pl.semaphore_signal(sem, inc=1, device_id=(1 - core, y, z, x), device_id_type=MESH)
    lax.fori_loop(1, 8, line, 0)
    lax.fori_loop(1, 16, plane, 0)
    pl.semaphore_wait(sem, 1 + 7 + 15)


def kernel(
    block, targets, weight, tangent, ggn, loss,
    held, lent, staged, turned, near_part, far_part, got_part, plane, line, terms, total,
    send_sems, recv_sems, load_sems, part_sems, plane_sems, line_sems, term_sems,
):
    core, y, z, x = (lax.axis_index(a) for a in ("seq",) + VOCAB)
    loads = [
        pltpu.make_async_copy(source, staged.at[k], load_sems.at[k]) for k, source in enumerate((weight, tangent))
    ]
    for copy in loads:
        copy.start()
    greet()
    net = Gather(block, held, lent, send_sems, recv_sems)
    net.start()
    partner = (1 - core, y, z, x)
    copies = []

    def turn(first, last):
        def chunk(i, carry):
            tile, at = i // 4, lax.rem(i, 4)
            chips = pl.ds(16 * at, 16)
            rows = pl.ds(pl.multiple_of(tile * 16, 16), 16)
            lanes = pl.ds(pl.multiple_of(at * 256, 256), 256)
            turned[tile, 0:WIDTH, lanes] = staged[0, chips, rows, :].reshape(256, WIDTH).T
            turned[tile, WIDTH : 2 * WIDTH, lanes] = staged[1, chips, rows, :].reshape(256, WIDTH).T
            return carry

        lax.fori_loop(first, last, chunk, 0)

    def logits(g, part):
        net.take(lent.at[g, :, :, :, net.rows(g, part)], "lend", g, part)
        ends = (0, *CUTS[g], ROWS)

        def deep(tile, carry):
            rows = pl.ds(pl.multiple_of(tile * 16, 16), 16)
            own = held[g, pl.ds(2 * core, 2), :, :, rows, :].reshape(1024, LANES)
            other = lent[g, :, :, :, rows, :].reshape(1024, LANES)
            product = jnp.dot(turned[tile], jnp.concatenate([own, other], axis=1), preferred_element_type=F32)
            near_part[g] += product[:, :LANES]
            far_part[g] += product[:, LANES:]
            return carry

        lax.fori_loop(ends[part] // 16, ends[part + 1] // 16 + core // 2, deep, 0)

    def exchange(g):
        copy = pltpu.make_async_remote_copy(
            src_ref=far_part.at[g], dst_ref=got_part.at[g], send_sem=part_sems.at[0, g], recv_sem=part_sems.at[1, g],
            device_id=partner, device_id_type=MESH,
        )
        copy.start()
        copies.append(copy)
        return copy

    def own_stats(g, copy):
        copy.wait_recv()
        values = near_part[g, 0:WIDTH] + got_part[g, 0:WIDTH]
        top = jnp.max(values, axis=0, keepdims=True)
        base = (y * 32 + z * 4 + x) * WIDTH
        ids = lax.broadcasted_iota(jnp.int32, (WIDTH, LANES), 0) + base
        picked = jnp.sum(jnp.where(ids == targets[g : g + 1, :], values, 0.0), axis=0, keepdims=True)
        exps = jnp.exp(values - top)
        near_part[g, 0:WIDTH] = exps
        tangents = near_part[g, WIDTH : 2 * WIDTH] + got_part[g, WIDTH : 2 * WIDTH]
        near_part[g, WIDTH : 2 * WIDTH] = tangents
        plane[g, 0, 0:1, :] = top
        plane[g, 0, 1:2, :] = jnp.sum(exps, axis=0, keepdims=True)
        plane[g, 0, 2:3, :] = jnp.sum(exps * tangents, axis=0, keepdims=True)
        plane[g, 0, 3:4, :] = picked
        plane[g, 0, 4:8, :] = jnp.zeros((4, LANES), F32)

        def give(i, carry):
            pltpu.make_async_remote_copy(
                src_ref=plane.at[g, 0], dst_ref=plane.at[g, i], send_sem=plane_sems.at[0, g],
                recv_sem=plane_sems.at[1, g],
                device_id=(core, lax.rem(y + i // 4, 4), z, lax.rem(x + lax.rem(i, 4), 4)), device_id_type=MESH,
            ).start()
            return carry

        lax.fori_loop(1, 16, give, 0)

    def joined(ref):
        tops = ref[:, 0:1, :]
        top = jnp.max(tops, axis=0)
        scale = jnp.exp(tops - top[None])
        sums = [jnp.sum(ref[:, k : k + 1, :] * scale, axis=0) for k in (1, 2)]
        return top, *sums, jnp.sum(ref[:, 3:4, :], axis=0)

    def plane_stats(g):
        every = plane.at[g, 1:16]
        pltpu.make_async_copy(every, every, plane_sems.at[1, g]).wait()
        for k, row in enumerate(joined(plane.at[g])):
            line[g, 0, k : k + 1, :] = row
        line[g, 0, 4:8, :] = jnp.zeros((4, LANES), F32)

        def give(i, carry):
            pltpu.make_async_remote_copy(
                src_ref=line.at[g, 0], dst_ref=line.at[g, i], send_sem=line_sems.at[0, g],
                recv_sem=line_sems.at[1, g], device_id=(core, y, lax.rem(z + i, 8), x), device_id_type=MESH,
            ).start()
            return carry

        lax.fori_loop(1, 8, give, 0)

    def term(g):
        every = line.at[g, 1:8]
        pltpu.make_async_copy(every, every, line_sems.at[1, g]).wait()
        top, totals, tangent_sum, picked = joined(line.at[g])
        loss[:, g * LANES : (g + 1) * LANES] = top + jnp.log(totals) - picked
        scale = jnp.exp(plane[g, 0, 0:1, :] - top) / totals
        expect = tangent_sum / totals
        value = near_part[g, 0:WIDTH] * scale * (near_part[g, WIDTH : 2 * WIDTH] - expect)
        terms[g, 0] = value.T.astype(BF16)
        copy = pltpu.make_async_remote_copy(
            src_ref=terms.at[g, 0], dst_ref=terms.at[g, 1], send_sem=term_sems.at[0, g], recv_sem=term_sems.at[1, g],
            device_id=partner, device_id_type=MESH,
        )
        copy.start()
        copies.append(copy)
        return copy

    def product(i, groups):
        half, zs = i // 4, pl.ds(2 * lax.rem(i, 4), 2)
        left, right = [], []
        for g in groups:
            left += [held[g, 2 * core + half, zs].reshape(512, LANES), lent[g, half, zs].reshape(512, LANES)]
            right += [terms[g, 0], terms[g, 1]]
        left, right = jnp.concatenate(left, axis=1), jnp.concatenate(right, axis=0)
        return jnp.dot(left, right, preferred_element_type=F32)

    def early(groups, i, carry):
        total[pl.ds(pl.multiple_of(i * 512, 512), 512)] = product(i, groups)
        return carry

    def last(groups, i, carry):
        rows = pl.ds(pl.multiple_of(i * 512, 512), 512)
        ggn[rows] = (total[rows] + product(i, groups)).astype(BF16)
        return carry

    for copy in loads:
        copy.wait()
    near_part[...] = jnp.zeros_like(near_part)
    far_part[...] = jnp.zeros_like(far_part)
    turn(0, 16)
    todo = {g: 3 for g in range(GROUPS)}
    parts, sent, clock = {}, {}, 0.0
    stages = []

    def advance(g, stage):
        nonlocal clock
        clock += 0.5
        if stage == 0:
            own_stats(g, parts[g])
        elif stage == 1:
            plane_stats(g)
        else:
            sent[g] = term(g)
            return
        stages.append((clock + 3.4, g, stage + 1))

    for kind, *rest in ORDER:
        if kind != LOGITS:
            net.event(kind, *rest)
            continue
        while stages and min(stages)[0] <= clock:
            stages.remove(first := min(stages))
            advance(*first[1:])
        logits(*rest)
        g, part = rest
        ends = (0, *CUTS[g], ROWS)
        clock += 0.045 * (ends[part + 1] - ends[part])
        todo[g] -= 1
        if todo[g] == 0:
            parts[g] = exchange(g)
            stages.append((clock + 1.4, g, 0))
    done = ()
    while stages:
        stages.remove(first := min(stages))
        if not done and not stages and first[2] == 2:
            done = tuple(sent)
            for g in done:
                sent[g].wait_recv()
            lax.fori_loop(0, 8, functools.partial(early, done), 0)
            clock += 1.5 * len(done)
        clock = max(clock, first[0])
        advance(*first[1:])
    rest = tuple(g for g in range(GROUPS) if g not in done)
    for g in rest:
        sent[g].wait_recv()
    lax.fori_loop(0, 8, functools.partial(last, rest), 0)
    net.finish(total)
    for copy in copies:
        copy.wait_send()
    for g in range(GROUPS):
        for sems, ref in ((plane_sems, plane.at[g, 1:16]), (line_sems, line.at[g, 1:8])):
            pltpu.make_async_copy(ref, ref, sems.at[0, g]).wait()


def on_device(hidden, weight, tangent, targets):
    block = hidden.T
    weight, tangent = (w.reshape(64, ROWS, WIDTH) for w in (weight, tangent))
    vmem, hbm = pl.BlockSpec(memory_space=pltpu.VMEM), pl.BlockSpec(memory_space=pl.ANY)
    dma = pltpu.SemaphoreType.DMA
    ggn, loss = pl.pallas_call(
        kernel,
        out_shape=(
            pltpu.VMEM((HALF, WIDTH), BF16),
            pltpu.VMEM((1, GROUPS * LANES), F32),
        ),
        in_specs=[vmem, vmem, hbm, hbm],
        out_specs=(vmem, vmem),
        scratch_shapes=[
            pltpu.VMEM((GROUPS, 4, 8, 4, ROWS, LANES), BF16),
            pltpu.VMEM((GROUPS, 2, 8, 4, ROWS, LANES), BF16),
            pltpu.VMEM((2, 64, ROWS, WIDTH), BF16),
            pltpu.VMEM((4, 2 * WIDTH, 1024), BF16),
            pltpu.VMEM((GROUPS, 2 * WIDTH, LANES), F32),
            pltpu.VMEM((GROUPS, 2 * WIDTH, LANES), F32),
            pltpu.VMEM((GROUPS, 2 * WIDTH, LANES), F32),
            pltpu.VMEM((GROUPS, 16, 8, LANES), F32),
            pltpu.VMEM((GROUPS, 8, 8, LANES), F32),
            pltpu.VMEM((GROUPS, 2, LANES, WIDTH), BF16),
            pltpu.VMEM((HALF, WIDTH), F32),
            dma((GROUPS,)),
            dma((ARRIVALS,)),
            dma((2,)),
            dma((2, GROUPS)),
            dma((2, GROUPS)),
            dma((2, GROUPS)),
            dma((2, GROUPS)),
        ],
        compiler_params=pltpu.CompilerParams(
            collective_id=0, has_side_effects=True, vmem_limit_bytes=52 * 2**20
        ),
        name="head_product",
    )(block, targets.reshape(GROUPS, LANES), weight, tangent)
    return ggn, loss.reshape(-1)


ARRIVALS = 144


def solution(mesh):
    split = Mesh(
        mesh.devices.reshape(mesh.shape["seq"], 4, 8, 4), ("seq", "vocab_0", "vocab_1", "vocab_2")
    )
    placed = (P("seq", VOCAB), P("seq", VOCAB), P("seq", VOCAB), P("seq"))
    return jax.shard_map(
        on_device,
        mesh=split,
        in_specs=placed,
        out_specs=(P("seq", VOCAB), P("seq")),
        check_vma=False,
    )
```

```python
import functools
import math

import jax
import jax.numpy as jnp
from jax import lax
from jax.experimental import pallas as pl
from jax.experimental.pallas import tpu as pltpu
from jax.sharding import Mesh
from jax.sharding import PartitionSpec as P

VOCAB = ("vocab_0", "vocab_1", "vocab_2")
MESH = pl.DeviceIdType.MESH
F32, BF16 = jnp.float32, jnp.bfloat16
GROUPS, LANES, ROWS, WIDTH, HALF = 4, 128, 64, 512, 4096
CUTS = ((32, 48), (16, 32), (16, 48), (16, 32))
PLANE, LINE_Z, RING_Z, FAR_Z, LINE_Y, RING_X, FAR_X, LINE_X, RING_Y, FAR_Y, LOGITS, START, STAGE, EARLY = range(14)
ORDER = (
    (0, 0), (1, 0), (1, 1), (0, 1), (4, 0, 3), (7, 0, 3), (8, 0, 0, -1), (5, 0, 0, -1), (7, 0, 1), (4, 0, 1), (4, 1,
    3), (7, 0, 2), (2, 0, 1, -1), (4, 0, 2), (8, 0, 0, 1), (2, 0, 1, 1), (5, 0, 0, 1), (7, 1, 3), (11, 2), (5, 1, 0,
    -1), (8, 1, 0, -1), (2, 1, 1, -1), (2, 1, 1, 1), (5, 0, 3, -1), (8, 0, 3, -1), (4, 1, 1), (4, 1, 2), (5, 0, 1,
    -1), (11, 3), (8, 0, 1, -1), (7, 1, 2), (5, 1, 3, -1), (8, 0, 2, -1), (8, 1, 0, 1), (2, 0, 2, -1), (5, 0, 2, -1),
    (7, 1, 1), (8, 0, 3, 1), (8, 1, 3, -1), (2, 0, 2, 1), (5, 1, 0, 1), (8, 0, 1, 1), (5, 1, 1, -1), (8, 0, 2, 1), (5,
    0, 3, 1), (5, 1, 2, -1), (5, 0, 1, 1), (2, 1, 2, -1), (8, 1, 3, 1), (5, 1, 3, 1), (1, 2), (5, 0, 2, 1), (2, 1, 2,
    1), (8, 1, 2, -1), (8, 1, 1, -1), (5, 1, 1, 1), (7, 2, 3), (0, 2), (2, 0, 3, -1), (5, 1, 2, 1), (8, 1, 2, 1), (5,
    2, 0, -1), (1, 3), (4, 2, 3), (0, 3), (2, 1, 3, -1), (8, 2, 0, -1), (8, 1, 1, 1), (2, 0, 3, 1), (2, 2, 1, -1), (9,
    0), (8, 2, 3, -1), (7, 2, 1), (7, 2, 2), (7, 3, 3), (2, 1, 3, 1), (6, 0), (5, 3, 0, -1), (4, 3, 3), (10, 0, 2),
    (5, 2, 3, -1), (2, 2, 1, 1), (5, 2, 0, 1), (2, 3, 1, -1), (8, 3, 0, -1), (10, 0, 1), (2, 3, 1, 1), (6, 1), (4, 2,
    2), (3, 1), (3, 0), (5, 3, 3, -1), (8, 2, 1, -1), (2, 2, 2, -1), (4, 2, 1), (8, 2, 2, -1), (8, 2, 0, 1), (8, 3, 3,
    -1), (8, 2, 3, 1), (2, 3, 2, -1), (7, 3, 2), (2, 2, 2, 1), (10, 1, 1), (10, 1, 0), (7, 3, 1), (5, 2, 2, -1), (10,
    0, 0), (5, 3, 0, 1), (2, 2, 3, -1), (2, 3, 2, 1), (4, 3, 1), (4, 3, 2), (9, 1), (5, 2, 3, 1), (2, 2, 3, 1), (5, 2,
    1, -1), (8, 3, 2, -1), (2, 3, 3, -1), (8, 3, 0, 1), (5, 3, 3, 1), (8, 3, 1, -1), (8, 2, 1, 1), (8, 2, 2, 1), (5,
    2, 2, 1), (5, 3, 1, -1), (2, 3, 3, 1), (5, 3, 2, -1), (10, 1, 2), (12, 0, 0), (3, 2), (8, 3, 3, 1), (5, 2, 1, 1),
    (5, 3, 1, 1), (5, 3, 2, 1), (3, 3), (8, 3, 2, 1), (8, 3, 1, 1), (10, 2, 0), (6, 2), (10, 3, 0), (12, 1, 0), (6,
    3), (9, 2), (10, 2, 1), (12, 0, 1), (9, 3), (10, 3, 1), (10, 2, 2), (10, 3, 2), (12, 1, 1), (12, 2, 0), (12, 0,
    2), (12, 3, 0), (13,), (12, 1, 2), (12, 2, 1), (12, 3, 1), (13,), (12, 2, 2), (12, 3, 2),
)


class Gather:
    def __init__(self, block, held, lent, send_sems, recv_sems):
        self.block, self.held, self.lent = block, held, lent
        self.send_sems, self.recv_sems = send_sems, recv_sems
        self.core, self.y, self.z, self.x = (lax.axis_index(a) for a in ("seq",) + VOCAB)
        self.names, self.sent = {}, [0] * GROUPS
        self.left = {}
        for kind, *rest in ORDER:
            if kind < LOGITS:
                key = rest[0], self.part(kind)
                self.left[key] = self.left.get(key, 0) + 1

    @staticmethod
    def part(kind):
        if kind in (PLANE, RING_Z, FAR_Z):
            return 0
        return 1 if kind in (LINE_Y, RING_X, FAR_X) else 2

    def rows(self, group, part):
        ends = (0, *CUTS[group], ROWS)
        return pl.ds(ends[part], ends[part + 1] - ends[part])

    def near(self, axis, step):
        at, count = {"y": (self.y, 4), "z": (self.z, 8), "x": (self.x, 4)}[axis]
        return lax.rem(at + step + count, count)

    def chip(self, **steps):
        return (self.core, *(self.near(a, steps.get(a, 0)) for a in "yzx"))

    def arrival(self, *name):
        if name not in self.names:
            self.names[name] = len(self.names)
        return self.recv_sems.at[self.names[name]]

    def send(self, source, target, name, device, cond=None, counted=True):
        group = name[1]
        copy = pltpu.make_async_remote_copy(
            src_ref=source,
            dst_ref=target,
            send_sem=self.send_sems.at[group],
            recv_sem=self.arrival(*name),
            device_id=device,
            device_id_type=MESH,
        )
        if counted:
            self.sent[group] += math.prod(target.shape[:-1])
        if cond is None:
            copy.start()
        else:
            pl.when(cond)(copy.start)

    def take(self, ref, *name):
        pltpu.make_async_copy(ref, ref, self.arrival(*name)).wait()

    def ring(self, ref, axis, kind, group, piece, steps=(1, -1)):
        for step in steps:
            self.send(ref, ref, (kind, group, piece, step), self.chip(**{axis: step}))

    def start(self, group):
        lanes = pl.ds(group * LANES, LANES)
        rest = pl.ds(CUTS[group][0], ROWS - CUTS[group][0])
        source = self.block.at[rest, lanes]
        target = self.held.at[group, self.y, self.z, self.x, rest]
        for step in (4, 3, 5, 2, 6, 1, 7):
            self.send(source, target, (LINE_Z, group), self.chip(z=step))
        pltpu.make_async_copy(source, target, self.arrival(LINE_Z, group)).start()
        first = self.rows(group, 0)
        source = self.block.at[first, lanes]
        target = self.held.at[group, self.y, self.z, self.x, first]
        for dy in (2, 1, 3, 0):
            for dx in (2, 1, 3, 0):
                if dy or dx:
                    self.send(source, target, (PLANE, group), self.chip(y=dy, x=dx))
        pltpu.make_async_copy(source, target, self.arrival(PLANE, group)).start()

    def event(self, kind, group, piece=0, step=0):
        held = self.held
        rows = self.rows(group, self.part(kind))
        if kind == PLANE:
            ref = held.at[group, :, self.z, :, rows]
            self.take(ref, PLANE, group)
            self.ring(ref, "z", RING_Z, group, 1)
        elif kind == LINE_Z:
            rest = pl.ds(CUTS[group][0], ROWS - CUTS[group][0])
            self.take(held.at[group, self.y, :, self.x, rest], LINE_Z, group)
            along_x = held.at[group, self.y, :, self.x, self.rows(group, 1)]
            along_y = held.at[group, self.y, :, self.x, self.rows(group, 2)]
            for hop in (2, 1, 3):
                self.send(along_y, along_y, (LINE_X, group, hop), self.chip(x=hop))
                self.send(along_x, along_x, (LINE_Y, group, hop), self.chip(y=hop))
            self.ring(along_y, "y", RING_Y, group, 0)
            self.ring(along_x, "x", RING_X, group, 0)
        elif kind == RING_Z:
            ref = held.at[group, :, self.near("z", -step * piece), :, rows]
            self.take(ref, RING_Z, group, piece, step)
            if piece < 3:
                self.ring(ref, "z", RING_Z, group, piece + 1, (step,))
            else:
                self.far(ref, "z", FAR_Z, group, 0, step)
        elif kind == FAR_Z:
            self.take(held.at[group, :, self.near("z", 4), :, rows], FAR_Z, group)
        elif kind == LINE_Y:
            ref = held.at[group, self.near("y", -piece), :, self.x, rows]
            self.take(ref, LINE_Y, group, piece)
            self.ring(ref, "x", RING_X, group, piece)
        elif kind == LINE_X:
            ref = held.at[group, self.y, :, self.near("x", -piece), rows]
            self.take(ref, LINE_X, group, piece)
            self.ring(ref, "y", RING_Y, group, piece)
        elif kind == RING_X:
            ref = held.at[group, self.near("y", -piece), :, self.near("x", -step), rows]
            self.take(ref, RING_X, group, piece, step)
            self.far(ref, "x", FAR_X, group, piece, step)
        elif kind == RING_Y:
            ref = held.at[group, self.near("y", -step), :, self.near("x", -piece), rows]
            self.take(ref, RING_Y, group, piece, step)
            self.far(ref, "y", FAR_Y, group, piece, step)
        elif kind == FAR_X:
            self.take(held.at[group, :, :, self.near("x", 2), rows], FAR_X, group)
        elif kind == FAR_Y:
            self.take(held.at[group, self.near("y", 2), :, :, rows], FAR_Y, group)
        part = self.part(kind)
        self.left[group, part] -= 1
        if self.left[group, part] == 0:
            self.lend(group, part)

    def far(self, ref, axis, kind, group, piece, step):
        this_way = lax.rem(self.core + group + piece, 2) == (0 if step == 1 else 1)
        self.send(ref, ref, (kind, group), self.chip(**{axis: step}), this_way, step == 1)

    def lend(self, group, part):
        rows = self.rows(group, part)
        source = self.held.at[group, pl.ds(2 - 2 * self.core, 2), :, :, rows]
        target = self.lent.at[group, :, :, :, rows]
        self.send(source, target, ("lend", group, part), (1 - self.core, self.y, self.z, self.x))

    def finish(self, ref):
        for group, lines in enumerate(self.sent):
            every = ref.at[0 : lines * LANES * 2 // (WIDTH * 4)]
            pltpu.make_async_copy(every, every, self.send_sems.at[group]).wait()


def greet():
    core, y, z, x = (lax.axis_index(a) for a in ("seq",) + VOCAB)
    sem = pltpu.get_barrier_semaphore()

    def plane(i, carry):
        to = (core, lax.rem(y + i // 4, 4), z, lax.rem(x + lax.rem(i, 4), 4))
        pl.semaphore_signal(sem, inc=1, device_id=to, device_id_type=MESH)
        return carry

    def line(i, carry):
        pl.semaphore_signal(sem, inc=1, device_id=(core, y, lax.rem(z + i, 8), x), device_id_type=MESH)
        return carry

    pl.semaphore_signal(sem, inc=1, device_id=(1 - core, y, z, x), device_id_type=MESH)
    lax.fori_loop(1, 8, line, 0)
    lax.fori_loop(1, 16, plane, 0)
    pl.semaphore_wait(sem, 1 + 7 + 15)


def kernel(
    block, targets, weight, tangent, ggn, loss,
    held, lent, staged, turned, near_part, far_part, got_part, plane, line, terms, total,
    send_sems, recv_sems, load_sems, part_sems, plane_sems, line_sems, term_sems,
):
    core, y, z, x = (lax.axis_index(a) for a in ("seq",) + VOCAB)
    loads = [
        pltpu.make_async_copy(source, staged.at[k], load_sems.at[k]) for k, source in enumerate((weight, tangent))
    ]
    for copy in loads:
        copy.start()
    greet()
    net = Gather(block, held, lent, send_sems, recv_sems)
    for g in range(GROUPS):
        if (START, g) not in ORDER:
            net.start(g)
    partner = (1 - core, y, z, x)
    copies = []

    def turn(first, last):
        def chunk(i, carry):
            tile, at = i // 4, lax.rem(i, 4)
            chips = pl.ds(16 * at, 16)
            rows = pl.ds(pl.multiple_of(tile * 16, 16), 16)
            lanes = pl.ds(pl.multiple_of(at * 256, 256), 256)
            turned[tile, 0:WIDTH, lanes] = staged[0, chips, rows, :].reshape(256, WIDTH).T
            turned[tile, WIDTH : 2 * WIDTH, lanes] = staged[1, chips, rows, :].reshape(256, WIDTH).T
            return carry

        lax.fori_loop(first, last, chunk, 0)

    def logits(g, part):
        net.take(lent.at[g, :, :, :, net.rows(g, part)], "lend", g, part)
        ends = (0, *CUTS[g], ROWS)

        def deep(tile, carry):
            rows = pl.ds(pl.multiple_of(tile * 16, 16), 16)
            own = held[g, pl.ds(2 * core, 2), :, :, rows, :].reshape(1024, LANES)
            other = lent[g, :, :, :, rows, :].reshape(1024, LANES)
            product = jnp.dot(turned[tile], jnp.concatenate([own, other], axis=1), preferred_element_type=F32)
            near_part[g] += product[:, :LANES]
            far_part[g] += product[:, LANES:]
            return carry

        lax.fori_loop(ends[part] // 16, ends[part + 1] // 16 + core // 2, deep, 0)

    def exchange(g):
        copy = pltpu.make_async_remote_copy(
            src_ref=far_part.at[g], dst_ref=got_part.at[g], send_sem=part_sems.at[0, g], recv_sem=part_sems.at[1, g],
            device_id=partner, device_id_type=MESH,
        )
        copy.start()
        copies.append(copy)
        return copy

    def own_stats(g, copy):
        copy.wait_recv()
        values = near_part[g, 0:WIDTH] + got_part[g, 0:WIDTH]
        top = jnp.max(values, axis=0, keepdims=True)
        base = (y * 32 + z * 4 + x) * WIDTH
        ids = lax.broadcasted_iota(jnp.int32, (WIDTH, LANES), 0) + base
        picked = jnp.sum(jnp.where(ids == targets[g : g + 1, :], values, 0.0), axis=0, keepdims=True)
        exps = jnp.exp(values - top)
        near_part[g, 0:WIDTH] = exps
        tangents = near_part[g, WIDTH : 2 * WIDTH] + got_part[g, WIDTH : 2 * WIDTH]
        near_part[g, WIDTH : 2 * WIDTH] = tangents
        plane[g, 0, 0:1, :] = top
        plane[g, 0, 1:2, :] = jnp.sum(exps, axis=0, keepdims=True)
        plane[g, 0, 2:3, :] = jnp.sum(exps * tangents, axis=0, keepdims=True)
        plane[g, 0, 3:4, :] = picked
        plane[g, 0, 4:8, :] = jnp.zeros((4, LANES), F32)

        def give(i, carry):
            pltpu.make_async_remote_copy(
                src_ref=plane.at[g, 0], dst_ref=plane.at[g, i], send_sem=plane_sems.at[0, g],
                recv_sem=plane_sems.at[1, g],
                device_id=(core, lax.rem(y + i // 4, 4), z, lax.rem(x + lax.rem(i, 4), 4)), device_id_type=MESH,
            ).start()
            return carry

        lax.fori_loop(1, 16, give, 0)

    def joined(ref):
        tops = ref[:, 0:1, :]
        top = jnp.max(tops, axis=0)
        scale = jnp.exp(tops - top[None])
        sums = [jnp.sum(ref[:, k : k + 1, :] * scale, axis=0) for k in (1, 2)]
        return top, *sums, jnp.sum(ref[:, 3:4, :], axis=0)

    def plane_stats(g):
        every = plane.at[g, 1:16]
        pltpu.make_async_copy(every, every, plane_sems.at[1, g]).wait()
        for k, row in enumerate(joined(plane.at[g])):
            line[g, 0, k : k + 1, :] = row
        line[g, 0, 4:8, :] = jnp.zeros((4, LANES), F32)

        def give(i, carry):
            pltpu.make_async_remote_copy(
                src_ref=line.at[g, 0], dst_ref=line.at[g, i], send_sem=line_sems.at[0, g],
                recv_sem=line_sems.at[1, g], device_id=(core, y, lax.rem(z + i, 8), x), device_id_type=MESH,
            ).start()
            return carry

        lax.fori_loop(1, 8, give, 0)

    def term(g):
        every = line.at[g, 1:8]
        pltpu.make_async_copy(every, every, line_sems.at[1, g]).wait()
        top, totals, tangent_sum, picked = joined(line.at[g])
        loss[:, g * LANES : (g + 1) * LANES] = top + jnp.log(totals) - picked
        scale = jnp.exp(plane[g, 0, 0:1, :] - top) / totals
        expect = tangent_sum / totals
        value = near_part[g, 0:WIDTH] * scale * (near_part[g, WIDTH : 2 * WIDTH] - expect)
        terms[g, 0] = value.T.astype(BF16)
        copy = pltpu.make_async_remote_copy(
            src_ref=terms.at[g, 0], dst_ref=terms.at[g, 1], send_sem=term_sems.at[0, g], recv_sem=term_sems.at[1, g],
            device_id=partner, device_id_type=MESH,
        )
        copy.start()
        copies.append(copy)
        return copy

    def product(i, groups):
        half, zs = i // 4, pl.ds(2 * lax.rem(i, 4), 2)
        left, right = [], []
        for g in groups:
            left += [held[g, 2 * core + half, zs].reshape(512, LANES), lent[g, half, zs].reshape(512, LANES)]
            right += [terms[g, 0], terms[g, 1]]
        left, right = jnp.concatenate(left, axis=1), jnp.concatenate(right, axis=0)
        return jnp.dot(left, right, preferred_element_type=F32)

    def early(groups, more, i, carry):
        rows = pl.ds(pl.multiple_of(i * 512, 512), 512)
        total[rows] = total[rows] + product(i, groups) if more else product(i, groups)
        return carry

    def last(groups, i, carry):
        rows = pl.ds(pl.multiple_of(i * 512, 512), 512)
        ggn[rows] = (total[rows] + product(i, groups)).astype(BF16)
        return carry

    for copy in loads:
        copy.wait()
    near_part[...] = jnp.zeros_like(near_part)
    far_part[...] = jnp.zeros_like(far_part)
    turn(0, 16)
    todo = {g: 3 for g in range(GROUPS)}
    parts, sent, done = {}, {}, ()
    for kind, *rest in ORDER:
        if kind == START:
            net.start(*rest)
        elif kind == LOGITS:
            logits(*rest)
            todo[rest[0]] -= 1
            if todo[rest[0]] == 0:
                parts[rest[0]] = exchange(rest[0])
        elif kind == STAGE:
            g, stage = rest
            if stage == 0:
                own_stats(g, parts[g])
            elif stage == 1:
                plane_stats(g)
            else:
                sent[g] = term(g)
        elif kind == EARLY:
            some = tuple(g for g in sent if g not in done)
            for g in some:
                sent[g].wait_recv()
            lax.fori_loop(0, 8, functools.partial(early, some, bool(done)), 0)
            done += some
        else:
            net.event(kind, *rest)
    rest = tuple(g for g in range(GROUPS) if g not in done)
    for g in rest:
        sent[g].wait_recv()
    lax.fori_loop(0, 8, functools.partial(last, rest), 0)
    net.finish(total)
    for copy in copies:
        copy.wait_send()
    for g in range(GROUPS):
        for sems, ref in ((plane_sems, plane.at[g, 1:16]), (line_sems, line.at[g, 1:8])):
            pltpu.make_async_copy(ref, ref, sems.at[0, g]).wait()


def on_device(hidden, weight, tangent, targets):
    block = hidden.T
    weight, tangent = (w.reshape(64, ROWS, WIDTH) for w in (weight, tangent))
    vmem, hbm = pl.BlockSpec(memory_space=pltpu.VMEM), pl.BlockSpec(memory_space=pl.ANY)
    dma = pltpu.SemaphoreType.DMA
    ggn, loss = pl.pallas_call(
        kernel,
        out_shape=(
            pltpu.VMEM((HALF, WIDTH), BF16),
            pltpu.VMEM((1, GROUPS * LANES), F32),
        ),
        in_specs=[vmem, vmem, hbm, hbm],
        out_specs=(vmem, vmem),
        scratch_shapes=[
            pltpu.VMEM((GROUPS, 4, 8, 4, ROWS, LANES), BF16),
            pltpu.VMEM((GROUPS, 2, 8, 4, ROWS, LANES), BF16),
            pltpu.VMEM((2, 64, ROWS, WIDTH), BF16),
            pltpu.VMEM((4, 2 * WIDTH, 1024), BF16),
            pltpu.VMEM((GROUPS, 2 * WIDTH, LANES), F32),
            pltpu.VMEM((GROUPS, 2 * WIDTH, LANES), F32),
            pltpu.VMEM((GROUPS, 2 * WIDTH, LANES), F32),
            pltpu.VMEM((GROUPS, 16, 8, LANES), F32),
            pltpu.VMEM((GROUPS, 8, 8, LANES), F32),
            pltpu.VMEM((GROUPS, 2, LANES, WIDTH), BF16),
            pltpu.VMEM((HALF, WIDTH), F32),
            dma((GROUPS,)),
            dma((ARRIVALS,)),
            dma((2,)),
            dma((2, GROUPS)),
            dma((2, GROUPS)),
            dma((2, GROUPS)),
            dma((2, GROUPS)),
        ],
        compiler_params=pltpu.CompilerParams(
            collective_id=0, has_side_effects=True, vmem_limit_bytes=52 * 2**20
        ),
        name="head_product",
    )(block, targets.reshape(GROUPS, LANES), weight, tangent)
    return ggn, loss.reshape(-1)


ARRIVALS = 144


def solution(mesh):
    split = Mesh(
        mesh.devices.reshape(mesh.shape["seq"], 4, 8, 4), ("seq", "vocab_0", "vocab_1", "vocab_2")
    )
    placed = (P("seq", VOCAB), P("seq", VOCAB), P("seq", VOCAB), P("seq"))
    return jax.shard_map(
        on_device,
        mesh=split,
        in_specs=placed,
        out_specs=(P("seq", VOCAB), P("seq")),
        check_vma=False,
    )
```

```python
import functools
import math

import jax
import jax.numpy as jnp
from jax import lax
from jax.experimental import pallas as pl
from jax.experimental.pallas import tpu as pltpu
from jax.sharding import Mesh
from jax.sharding import PartitionSpec as P

VOCAB = ("vocab_0", "vocab_1", "vocab_2")
MESH = pl.DeviceIdType.MESH
F32, BF16 = jnp.float32, jnp.bfloat16
GROUPS, LANES, ROWS, WIDTH, HALF = 4, 128, 64, 512, 4096
CUTS = ((32, 48), (16, 32), (16, 48), (16, 32))
PLANE, LINE_Z, RING_Z, FAR_Z, LINE_Y, RING_X, FAR_X, LINE_X, RING_Y, FAR_Y, LOGITS, START, STAGE, EARLY = range(14)
ORDER = (
    (0, 0), (1, 0), (1, 1), (0, 1), (4, 0, 3), (7, 0, 3), (8, 0, 0, -1), (5, 0, 0, -1), (7, 0, 1), (4, 0, 1), (4, 1,
    3), (7, 0, 2), (2, 0, 1, -1), (4, 0, 2), (8, 0, 0, 1), (2, 0, 1, 1), (5, 0, 0, 1), (7, 1, 3), (11, 2), (5, 1, 0,
    -1), (8, 1, 0, -1), (2, 1, 1, -1), (2, 1, 1, 1), (5, 0, 3, -1), (8, 0, 3, -1), (4, 1, 1), (4, 1, 2), (5, 0, 1,
    -1), (11, 3), (8, 0, 1, -1), (7, 1, 2), (5, 1, 3, -1), (8, 0, 2, -1), (8, 1, 0, 1), (2, 0, 2, -1), (5, 0, 2, -1),
    (7, 1, 1), (8, 0, 3, 1), (8, 1, 3, -1), (2, 0, 2, 1), (5, 1, 0, 1), (8, 0, 1, 1), (5, 1, 1, -1), (8, 0, 2, 1), (5,
    0, 3, 1), (5, 1, 2, -1), (5, 0, 1, 1), (2, 1, 2, -1), (8, 1, 3, 1), (5, 1, 3, 1), (1, 2), (5, 0, 2, 1), (2, 1, 2,
    1), (8, 1, 2, -1), (8, 1, 1, -1), (5, 1, 1, 1), (7, 2, 3), (0, 2), (2, 0, 3, -1), (5, 1, 2, 1), (8, 1, 2, 1), (5,
    2, 0, -1), (1, 3), (4, 2, 3), (0, 3), (2, 1, 3, -1), (8, 2, 0, -1), (8, 1, 1, 1), (2, 0, 3, 1), (2, 2, 1, -1), (9,
    0), (8, 2, 3, -1), (7, 2, 1), (7, 2, 2), (7, 3, 3), (2, 1, 3, 1), (6, 0), (5, 3, 0, -1), (4, 3, 3), (10, 0, 2),
    (5, 2, 3, -1), (2, 2, 1, 1), (5, 2, 0, 1), (2, 3, 1, -1), (8, 3, 0, -1), (10, 0, 1), (2, 3, 1, 1), (6, 1), (4, 2,
    2), (3, 1), (3, 0), (5, 3, 3, -1), (8, 2, 1, -1), (2, 2, 2, -1), (4, 2, 1), (8, 2, 2, -1), (8, 2, 0, 1), (8, 3, 3,
    -1), (8, 2, 3, 1), (2, 3, 2, -1), (7, 3, 2), (2, 2, 2, 1), (10, 1, 1), (10, 1, 0), (7, 3, 1), (5, 2, 2, -1), (10,
    0, 0), (5, 3, 0, 1), (2, 2, 3, -1), (2, 3, 2, 1), (4, 3, 1), (4, 3, 2), (9, 1), (5, 2, 3, 1), (2, 2, 3, 1), (5, 2,
    1, -1), (8, 3, 2, -1), (2, 3, 3, -1), (8, 3, 0, 1), (5, 3, 3, 1), (8, 3, 1, -1), (8, 2, 1, 1), (8, 2, 2, 1), (5,
    2, 2, 1), (5, 3, 1, -1), (2, 3, 3, 1), (5, 3, 2, -1), (10, 1, 2), (12, 0, 0), (3, 2), (8, 3, 3, 1), (5, 2, 1, 1),
    (5, 3, 1, 1), (5, 3, 2, 1), (3, 3), (8, 3, 2, 1), (8, 3, 1, 1), (10, 2, 0), (6, 2), (10, 3, 0), (12, 1, 0), (6,
    3), (9, 2), (10, 2, 1), (12, 0, 1), (9, 3), (10, 3, 1), (10, 2, 2), (10, 3, 2), (12, 1, 1), (12, 2, 0), (12, 0,
    2), (12, 3, 0), (13,), (12, 1, 2), (12, 2, 1), (12, 3, 1), (13,), (12, 2, 2), (12, 3, 2),
)


class Gather:
    def __init__(self, block, held, lent, send_sems, recv_sems):
        self.block, self.held, self.lent = block, held, lent
        self.send_sems, self.recv_sems = send_sems, recv_sems
        self.core, self.y, self.z, self.x = (lax.axis_index(a) for a in ("seq",) + VOCAB)
        self.names, self.sent = {}, [0] * GROUPS
        self.left = {}
        for kind, *rest in ORDER:
            if kind < LOGITS:
                key = rest[0], self.part(kind)
                self.left[key] = self.left.get(key, 0) + 1

    @staticmethod
    def part(kind):
        if kind in (PLANE, RING_Z, FAR_Z):
            return 0
        return 1 if kind in (LINE_Y, RING_X, FAR_X) else 2

    def rows(self, group, part):
        ends = (0, *CUTS[group], ROWS)
        return pl.ds(ends[part], ends[part + 1] - ends[part])

    def near(self, axis, step):
        at, count = {"y": (self.y, 4), "z": (self.z, 8), "x": (self.x, 4)}[axis]
        return lax.rem(at + step + count, count)

    def chip(self, **steps):
        return (self.core, *(self.near(a, steps.get(a, 0)) for a in "yzx"))

    def arrival(self, *name):
        if name not in self.names:
            self.names[name] = len(self.names)
        return self.recv_sems.at[self.names[name]]

    def send(self, source, target, name, device, cond=None, counted=True):
        group = name[1]
        copy = pltpu.make_async_remote_copy(
            src_ref=source,
            dst_ref=target,
            send_sem=self.send_sems.at[group],
            recv_sem=self.arrival(*name),
            device_id=device,
            device_id_type=MESH,
        )
        if counted:
            self.sent[group] += math.prod(target.shape[:-1])
        if cond is None:
            copy.start()
        else:
            pl.when(cond)(copy.start)

    def take(self, ref, *name):
        pltpu.make_async_copy(ref, ref, self.arrival(*name)).wait()

    def ring(self, ref, axis, kind, group, piece, steps=(1, -1)):
        for step in steps:
            self.send(ref, ref, (kind, group, piece, step), self.chip(**{axis: step}))

    def start(self, group):
        lanes = pl.ds(group * LANES, LANES)
        rest = pl.ds(CUTS[group][0], ROWS - CUTS[group][0])
        source = self.block.at[rest, lanes]
        target = self.held.at[group, self.y, self.z, self.x, rest]
        for step in (4, 3, 5, 2, 6, 1, 7):
            self.send(source, target, (LINE_Z, group), self.chip(z=step))
        pltpu.make_async_copy(source, target, self.arrival(LINE_Z, group)).start()
        first = self.rows(group, 0)
        source = self.block.at[first, lanes]
        target = self.held.at[group, self.y, self.z, self.x, first]
        for dy in (2, 1, 3, 0):
            for dx in (2, 1, 3, 0):
                if dy or dx:
                    self.send(source, target, (PLANE, group), self.chip(y=dy, x=dx))
        pltpu.make_async_copy(source, target, self.arrival(PLANE, group)).start()

    def event(self, kind, group, piece=0, step=0):
        held = self.held
        rows = self.rows(group, self.part(kind))
        if kind == PLANE:
            ref = held.at[group, :, self.z, :, rows]
            self.take(ref, PLANE, group)
            self.ring(ref, "z", RING_Z, group, 1)
        elif kind == LINE_Z:
            rest = pl.ds(CUTS[group][0], ROWS - CUTS[group][0])
            self.take(held.at[group, self.y, :, self.x, rest], LINE_Z, group)
            along_x = held.at[group, self.y, :, self.x, self.rows(group, 1)]
            along_y = held.at[group, self.y, :, self.x, self.rows(group, 2)]
            for hop in (2, 1, 3):
                self.send(along_y, along_y, (LINE_X, group, hop), self.chip(x=hop))
                self.send(along_x, along_x, (LINE_Y, group, hop), self.chip(y=hop))
            self.ring(along_y, "y", RING_Y, group, 0)
            self.ring(along_x, "x", RING_X, group, 0)
        elif kind == RING_Z:
            ref = held.at[group, :, self.near("z", -step * piece), :, rows]
            self.take(ref, RING_Z, group, piece, step)
            if piece < 3:
                self.ring(ref, "z", RING_Z, group, piece + 1, (step,))
            else:
                self.far(ref, "z", FAR_Z, group, 0, step)
        elif kind == FAR_Z:
            self.take(held.at[group, :, self.near("z", 4), :, rows], FAR_Z, group)
        elif kind == LINE_Y:
            ref = held.at[group, self.near("y", -piece), :, self.x, rows]
            self.take(ref, LINE_Y, group, piece)
            self.ring(ref, "x", RING_X, group, piece)
        elif kind == LINE_X:
            ref = held.at[group, self.y, :, self.near("x", -piece), rows]
            self.take(ref, LINE_X, group, piece)
            self.ring(ref, "y", RING_Y, group, piece)
        elif kind == RING_X:
            ref = held.at[group, self.near("y", -piece), :, self.near("x", -step), rows]
            self.take(ref, RING_X, group, piece, step)
            self.far(ref, "x", FAR_X, group, piece, step)
        elif kind == RING_Y:
            ref = held.at[group, self.near("y", -step), :, self.near("x", -piece), rows]
            self.take(ref, RING_Y, group, piece, step)
            self.far(ref, "y", FAR_Y, group, piece, step)
        elif kind == FAR_X:
            self.take(held.at[group, :, :, self.near("x", 2), rows], FAR_X, group)
        elif kind == FAR_Y:
            self.take(held.at[group, self.near("y", 2), :, :, rows], FAR_Y, group)
        part = self.part(kind)
        self.left[group, part] -= 1
        if self.left[group, part] == 0:
            self.lend(group, part)

    def far(self, ref, axis, kind, group, piece, step):
        this_way = lax.rem(self.core + group + piece, 2) == (0 if step == 1 else 1)
        self.send(ref, ref, (kind, group), self.chip(**{axis: step}), this_way, step == 1)

    def lend(self, group, part):
        rows = self.rows(group, part)
        source = self.held.at[group, pl.ds(2 - 2 * self.core, 2), :, :, rows]
        target = self.lent.at[group, :, :, :, rows]
        self.send(source, target, ("lend", group, part), (1 - self.core, self.y, self.z, self.x))

    def finish(self, ref):
        for group, lines in enumerate(self.sent):
            every = ref.at[0 : lines * LANES * 2 // (WIDTH * 4)]
            pltpu.make_async_copy(every, every, self.send_sems.at[group]).wait()


def greet():
    core, y, z, x = (lax.axis_index(a) for a in ("seq",) + VOCAB)
    sem = pltpu.get_barrier_semaphore()

    def plane(i, carry):
        to = (core, lax.rem(y + i // 4, 4), z, lax.rem(x + lax.rem(i, 4), 4))
        pl.semaphore_signal(sem, inc=1, device_id=to, device_id_type=MESH)
        return carry

    def line(i, carry):
        pl.semaphore_signal(sem, inc=1, device_id=(core, y, lax.rem(z + i, 8), x), device_id_type=MESH)
        return carry

    pl.semaphore_signal(sem, inc=1, device_id=(1 - core, y, z, x), device_id_type=MESH)
    lax.fori_loop(1, 8, line, 0)
    lax.fori_loop(1, 16, plane, 0)
    pl.semaphore_wait(sem, 1 + 7 + 15)


def kernel(
    block, targets, weight, tangent, ggn, loss,
    held, lent, staged, turned, near_part, far_part, got_part, plane, line, terms, total,
    send_sems, recv_sems, load_sems, part_sems, plane_sems, line_sems, term_sems,
):
    core, y, z, x = (lax.axis_index(a) for a in ("seq",) + VOCAB)
    loads = [
        pltpu.make_async_copy(source, staged.at[k], load_sems.at[k]) for k, source in enumerate((weight, tangent))
    ]
    for copy in loads:
        copy.start()
    greet()
    net = Gather(block, held, lent, send_sems, recv_sems)
    for g in range(GROUPS):
        if (START, g) not in ORDER:
            net.start(g)
    partner = (1 - core, y, z, x)
    copies = []

    def turn(first, last):
        def chunk(i, carry):
            tile, at = i // 4, lax.rem(i, 4)
            chips = pl.ds(16 * at, 16)
            rows = pl.ds(pl.multiple_of(tile * 16, 16), 16)
            lanes = pl.ds(pl.multiple_of(at * 256, 256), 256)
            turned[tile, 0:WIDTH, lanes] = staged[0, chips, rows, :].reshape(256, WIDTH).T
            turned[tile, WIDTH : 2 * WIDTH, lanes] = staged[1, chips, rows, :].reshape(256, WIDTH).T
            return carry

        lax.fori_loop(first, last, chunk, 0)

    def logits(g, part):
        net.take(lent.at[g, :, :, :, net.rows(g, part)], "lend", g, part)
        ends = (0, *CUTS[g], ROWS)

        def deep(tile, carry):
            rows = pl.ds(pl.multiple_of(tile * 16, 16), 16)
            own = held[g, pl.ds(2 * core, 2), :, :, rows, :].reshape(1024, LANES)
            other = lent[g, :, :, :, rows, :].reshape(1024, LANES)
            product = jnp.dot(turned[tile], jnp.concatenate([own, other], axis=1), preferred_element_type=F32)
            near_part[g] += product[:, :LANES]
            far_part[g] += product[:, LANES:]
            return carry

        lax.fori_loop(ends[part] // 16, ends[part + 1] // 16 + core // 2, deep, 0)

    def exchange(g):
        copy = pltpu.make_async_remote_copy(
            src_ref=far_part.at[g], dst_ref=got_part.at[g], send_sem=part_sems.at[0, g], recv_sem=part_sems.at[1, g],
            device_id=partner, device_id_type=MESH,
        )
        copy.start()
        copies.append(copy)
        return copy

    def own_stats(g, copy):
        copy.wait_recv()
        values = near_part[g, 0:WIDTH] + got_part[g, 0:WIDTH]
        top = jnp.max(values, axis=0, keepdims=True)
        base = (y * 32 + z * 4 + x) * WIDTH
        ids = lax.broadcasted_iota(jnp.int32, (WIDTH, LANES), 0) + base
        picked = jnp.sum(jnp.where(ids == targets[g : g + 1, :], values, 0.0), axis=0, keepdims=True)
        exps = jnp.exp(values - top)
        near_part[g, 0:WIDTH] = exps
        tangents = near_part[g, WIDTH : 2 * WIDTH] + got_part[g, WIDTH : 2 * WIDTH]
        near_part[g, WIDTH : 2 * WIDTH] = tangents
        plane[g, 0, 0:1, :] = top
        plane[g, 0, 1:2, :] = jnp.sum(exps, axis=0, keepdims=True)
        plane[g, 0, 2:3, :] = jnp.sum(exps * tangents, axis=0, keepdims=True)
        plane[g, 0, 3:4, :] = picked
        plane[g, 0, 4:8, :] = jnp.zeros((4, LANES), F32)

        def give(i, carry):
            pltpu.make_async_remote_copy(
                src_ref=plane.at[g, 0], dst_ref=plane.at[g, i], send_sem=plane_sems.at[0, g],
                recv_sem=plane_sems.at[1, g],
                device_id=(core, lax.rem(y + i // 4, 4), z, lax.rem(x + lax.rem(i, 4), 4)), device_id_type=MESH,
            ).start()
            return carry

        lax.fori_loop(1, 16, give, 0)

    def joined(ref):
        tops = ref[:, 0:1, :]
        top = jnp.max(tops, axis=0)
        scale = jnp.exp(tops - top[None])
        sums = [jnp.sum(ref[:, k : k + 1, :] * scale, axis=0) for k in (1, 2)]
        return top, *sums, jnp.sum(ref[:, 3:4, :], axis=0)

    def plane_stats(g):
        every = plane.at[g, 1:16]
        pltpu.make_async_copy(every, every, plane_sems.at[1, g]).wait()
        for k, row in enumerate(joined(plane.at[g])):
            line[g, 0, k : k + 1, :] = row
        line[g, 0, 4:8, :] = jnp.zeros((4, LANES), F32)

        def give(i, carry):
            pltpu.make_async_remote_copy(
                src_ref=line.at[g, 0], dst_ref=line.at[g, i], send_sem=line_sems.at[0, g],
                recv_sem=line_sems.at[1, g], device_id=(core, y, lax.rem(z + i, 8), x), device_id_type=MESH,
            ).start()
            return carry

        lax.fori_loop(1, 8, give, 0)

    def term(g):
        every = line.at[g, 1:8]
        pltpu.make_async_copy(every, every, line_sems.at[1, g]).wait()
        top, totals, tangent_sum, picked = joined(line.at[g])
        loss[:, g * LANES : (g + 1) * LANES] = top + jnp.log(totals) - picked
        scale = jnp.exp(plane[g, 0, 0:1, :] - top) / totals
        expect = tangent_sum / totals
        value = near_part[g, 0:WIDTH] * scale * (near_part[g, WIDTH : 2 * WIDTH] - expect)
        terms[g, 0] = value.T.astype(BF16)
        copy = pltpu.make_async_remote_copy(
            src_ref=terms.at[g, 0], dst_ref=terms.at[g, 1], send_sem=term_sems.at[0, g], recv_sem=term_sems.at[1, g],
            device_id=partner, device_id_type=MESH,
        )
        copy.start()
        copies.append(copy)
        return copy

    def product(i, groups):
        half, zs = i // 2, pl.ds(4 * lax.rem(i, 2), 4)
        left, right = [], []
        for g in groups:
            left += [held[g, 2 * core + half, zs].reshape(1024, LANES), lent[g, half, zs].reshape(1024, LANES)]
            right += [terms[g, 0], terms[g, 1]]
        left, right = jnp.concatenate(left, axis=1), jnp.concatenate(right, axis=0)
        return jnp.dot(left, right, preferred_element_type=F32)

    def early(groups, more, i, carry):
        rows = pl.ds(pl.multiple_of(i * 1024, 1024), 1024)
        total[rows] = total[rows] + product(i, groups) if more else product(i, groups)
        return carry

    def last(groups, i, carry):
        rows = pl.ds(pl.multiple_of(i * 1024, 1024), 1024)
        ggn[rows] = (total[rows] + product(i, groups)).astype(BF16)
        return carry

    for copy in loads:
        copy.wait()
    near_part[...] = jnp.zeros_like(near_part)
    far_part[...] = jnp.zeros_like(far_part)
    turn(0, 16)
    todo = {g: 3 for g in range(GROUPS)}
    parts, sent, done = {}, {}, ()
    for kind, *rest in ORDER:
        if kind == START:
            net.start(*rest)
        elif kind == LOGITS:
            logits(*rest)
            todo[rest[0]] -= 1
            if todo[rest[0]] == 0:
                parts[rest[0]] = exchange(rest[0])
        elif kind == STAGE:
            g, stage = rest
            if stage == 0:
                own_stats(g, parts[g])
            elif stage == 1:
                plane_stats(g)
            else:
                sent[g] = term(g)
        elif kind == EARLY:
            some = tuple(g for g in sent if g not in done)
            for g in some:
                sent[g].wait_recv()
            lax.fori_loop(0, 4, functools.partial(early, some, bool(done)), 0)
            done += some
        else:
            net.event(kind, *rest)
    rest = tuple(g for g in range(GROUPS) if g not in done)
    for g in rest:
        sent[g].wait_recv()
    lax.fori_loop(0, 4, functools.partial(last, rest), 0)
    net.finish(total)
    for copy in copies:
        copy.wait_send()
    for g in range(GROUPS):
        for sems, ref in ((plane_sems, plane.at[g, 1:16]), (line_sems, line.at[g, 1:8])):
            pltpu.make_async_copy(ref, ref, sems.at[0, g]).wait()


def on_device(hidden, weight, tangent, targets):
    block = hidden.T
    weight, tangent = (w.reshape(64, ROWS, WIDTH) for w in (weight, tangent))
    vmem, hbm = pl.BlockSpec(memory_space=pltpu.VMEM), pl.BlockSpec(memory_space=pl.ANY)
    dma = pltpu.SemaphoreType.DMA
    ggn, loss = pl.pallas_call(
        kernel,
        out_shape=(
            pltpu.VMEM((HALF, WIDTH), BF16),
            pltpu.VMEM((1, GROUPS * LANES), F32),
        ),
        in_specs=[vmem, vmem, hbm, hbm],
        out_specs=(vmem, vmem),
        scratch_shapes=[
            pltpu.VMEM((GROUPS, 4, 8, 4, ROWS, LANES), BF16),
            pltpu.VMEM((GROUPS, 2, 8, 4, ROWS, LANES), BF16),
            pltpu.VMEM((2, 64, ROWS, WIDTH), BF16),
            pltpu.VMEM((4, 2 * WIDTH, 1024), BF16),
            pltpu.VMEM((GROUPS, 2 * WIDTH, LANES), F32),
            pltpu.VMEM((GROUPS, 2 * WIDTH, LANES), F32),
            pltpu.VMEM((GROUPS, 2 * WIDTH, LANES), F32),
            pltpu.VMEM((GROUPS, 16, 8, LANES), F32),
            pltpu.VMEM((GROUPS, 8, 8, LANES), F32),
            pltpu.VMEM((GROUPS, 2, LANES, WIDTH), BF16),
            pltpu.VMEM((HALF, WIDTH), F32),
            dma((GROUPS,)),
            dma((ARRIVALS,)),
            dma((2,)),
            dma((2, GROUPS)),
            dma((2, GROUPS)),
            dma((2, GROUPS)),
            dma((2, GROUPS)),
        ],
        compiler_params=pltpu.CompilerParams(
            collective_id=0, has_side_effects=True, vmem_limit_bytes=52 * 2**20
        ),
        name="head_product",
    )(block, targets.reshape(GROUPS, LANES), weight, tangent)
    return ggn, loss.reshape(-1)


ARRIVALS = 144


def solution(mesh):
    split = Mesh(
        mesh.devices.reshape(mesh.shape["seq"], 4, 8, 4), ("seq", "vocab_0", "vocab_1", "vocab_2")
    )
    placed = (P("seq", VOCAB), P("seq", VOCAB), P("seq", VOCAB), P("seq"))
    return jax.shard_map(
        on_device,
        mesh=split,
        in_specs=placed,
        out_specs=(P("seq", VOCAB), P("seq")),
        check_vma=False,
    )
```
